512 devices in a mesh: groups: 2 (over y), ep: 32 (over z), tp: 4 (over x), dp: 2 (over core).
Axes of the slice: x: 4, y: 2, z: 32, core: 2. Of those that a mesh axis runs over, the one named last changes fastest.
The devices are a block of a 4x8x32 slice.
Arguments:
- tokens: bfloat16 [8192, 1536], P(('groups', 'ep', 'tp', 'dp')), parts along dimension 0, may hold values from -6 to 6
- expert_ids: int32 [8192, 4], P(('groups', 'ep', 'tp', 'dp')), parts along dimension 0, may hold values from 0 to 63, all different within a row; in each aligned block of 16 rows (0 to 15, 16 to 31, ...) at most 2 rows name the same one
- gate_weights: float32 [8192, 4], P(('groups', 'ep', 'tp', 'dp')), parts along dimension 0, may hold values from 0.1 to 1
- w_gate: bfloat16 [64, 1536, 1536], P(('ep', 'dp'), None, 'tp'), may hold values from -0.15625 to 0.15625
- w_up: bfloat16 [64, 1536, 1536], P(('ep', 'dp'), None, 'tp'), may hold values from -0.15625 to 0.15625
- w_down: bfloat16 [64, 1536, 1536], P(('ep', 'dp'), None, 'tp'), may hold values from -0.15625 to 0.15625
Outputs:
- mixed: bfloat16 [8192, 1536], P(('groups', 'ep', 'tp', 'dp')), parts along dimension 0
- expert_loads: int32 [128], P('groups'), parts along dimension 0
The draws below stay inside these ranges and needn't reach their ends.
There are 2 independent parts, one for each index of `groups`. The reference program is written for one: setup_inputs(seed, part) draws one part's arguments, and reference() takes and returns one part's arrays. A program takes and returns all parts, laid end to end along the dimension named above; an argument that names none is the same for every part. Nothing has to cross between parts.
Inputs may be any that keep to these rules, and one draw needn't show every extreme that they name: `expert_ids`: each row names 4 different experts. In each aligned block of 16 rows (the rows of one device) no expert is named by more than 2 rows, and in some blocks one expert is named by exactly 2 rows.
All inputs are finite; a program needn't handle non-finite values.
Results may differ from the reference program's by a relative error of at most 0.0057.
Values may be sent and summed in bfloat16 or wider, within the bound.
A program may use at most 64 MiB of HBM per device.

```python
import math
import jax
import jax.numpy as jnp
import numpy as np
from jax import lax

D = 1536
FF = 1536
TOP = 4
TOK_DEV = 16
EXPERTS = 64
CAP = 2
TOKENS = 4096


def level_of(rng, shape, shards, low, largest):
    gain = 1.0
    for position, parts in shards:
        steps = jax.random.uniform(jax.random.fold_in(jax.random.fold_in(rng, 6), position), (parts,), jnp.float32, low / len(shards), largest / len(shards))
        gain = gain * jnp.repeat(jnp.exp(steps), shape[position] // parts).reshape((-1,) + (1,) * (len(shape) - 1 - position))
    return gain


def shared_out(own_key, own, number, rows, amount, top, bound, slope):
    sequence = jax.random.permutation(own_key, amount)
    crowded, ordinary = portions_of(amount, rows * top, bound, slope, True), portions_of(amount, rows * top, bound, slope, False)
    places = jnp.arange(amount)

    def named(lengths, offset_by):
        used = int((lengths > 0).sum())
        fixed = max(1, used // 4)
        passed = fixed + (places - fixed + offset_by * (used - fixed)) % max(1, amount - fixed)
        return jnp.zeros((amount,), jnp.int32).at[sequence[jnp.where(places < fixed, places, passed)]].set(jnp.asarray(lengths, jnp.int32))

    lengths = jnp.where(number % 4 == 0, named(crowded, number // 4), named(ordinary, number - number // 4 - 1))
    mixed = jax.random.permutation(jax.random.fold_in(own, 3), amount)
    donor, receiver = mixed[0:amount // 2 * 2:2], mixed[1:amount // 2 * 2:2]
    slack = jnp.minimum(lengths[donor] - 1, bound - lengths[receiver]) // 2
    slack = jnp.where((donor == sequence[0]) | (receiver == sequence[0]) | (lengths[receiver] == 0), 0, jnp.maximum(slack, 0))
    passed = jax.random.randint(jax.random.fold_in(own, 4), (amount // 2,), 0, 1 << 20) % (slack + 1)
    lengths = lengths.at[donor].add(-passed).at[receiver].add(passed)
    labels = jnp.searchsorted(jnp.cumsum(lengths), jnp.arange(rows * top), side="right").astype(jnp.int32)
    table = labels.reshape(top, rows).T
    table = table[jax.random.permutation(jax.random.fold_in(own, 1), rows)]
    offset_by = jax.random.randint(jax.random.fold_in(own, 2), (rows, 1), 0, top)
    return jnp.take_along_axis(table, (jnp.arange(top)[None, :] + offset_by) % top, axis=1)


def portions_of(amount, total, limit, skew, full):
    portions = [(1 << 20) // math.isqrt(rank ** skew) + 1 for rank in range(1, amount + 1)]
    largest = limit if full else min(limit, max(-(-total // amount), total * portions[0] // sum(portions)))
    least = 1 if total - largest >= amount - 1 else 0
    given, surplus = [largest] + [least] * (amount - 1), total - largest - least * (amount - 1)
    while surplus > 0:
        candidates = [i for i in range(1, amount) if given[i] < largest] or [i for i in range(1, amount) if given[i] < limit]
        pool, left = sum([portions[i] for i in candidates]), surplus
        for i in candidates:
            more = min(limit - given[i], max(1, left * portions[i] // pool), surplus)
            given[i] = given[i] + more
            surplus = surplus - more
    return np.array(given)


def bell_draw(own_key, shape, spread, reach, cuts=(), held_as=jnp.bfloat16):
    values = jax.random.normal(own_key, shape, jnp.float32) * spread
    if len(cuts) > 0:
        values = level_of(own_key, shape, cuts, -0.22, 0.18) * values
    return jnp.clip(values, min=-reach, max=reach).astype(held_as)


def setup_inputs(seed: int = 0, part: int = 0) -> dict:
    key_of = jax.random.split(jax.random.key(seed), 7)
    own_keys = jax.random.split(jax.random.fold_in(key_of[6], part), 7)
    tokens = bell_draw(own_keys[0], (TOKENS, D), 1.0, 6.0, ((0, 256),))
    expert_ids_keys = jax.random.split(jax.random.fold_in(own_keys[1], 1), TOKENS // TOK_DEV)
    expert_ids_turns = jax.random.permutation(jax.random.fold_in(own_keys[1], 3), TOKENS // TOK_DEV)
    expert_ids = jax.vmap(lambda own, number: shared_out(jax.random.fold_in(own_keys[1], 2), own, number, TOK_DEV, EXPERTS, TOP, CAP, 2))(expert_ids_keys, expert_ids_turns).reshape((TOKENS, TOP))
    gate_weights = jnp.clip(0.1 + 0.9 * jax.random.uniform(own_keys[2], (TOKENS, TOP), jnp.float32) ** level_of(own_keys[2], (TOKENS, TOP), ((0, 256),), -0.2, 0.2), 0.1, 1.0)
    w_gate = bell_draw(key_of[3], (EXPERTS, D, FF), D ** -0.5, 0.15625, ((0, 64), (2, 4)))
    w_up = bell_draw(key_of[4], (EXPERTS, D, FF), D ** -0.5, 0.15625, ((0, 64), (2, 4)))
    w_down = bell_draw(key_of[5], (EXPERTS, D, FF), FF ** -0.5, 0.15625, ((0, 64), (2, 4)))
    return {"tokens": tokens, "expert_ids": expert_ids, "gate_weights": gate_weights, "w_gate": w_gate, "w_up": w_up, "w_down": w_down}


def reference(tokens, expert_ids, gate_weights, w_gate, w_up, w_down):
    pair_ids = expert_ids.reshape(-1).astype(jnp.int32)
    pair_count = pair_ids.shape[0]
    expert_range = jnp.arange(EXPERTS, dtype=jnp.int32)
    onehot = (pair_ids[:, None] == expert_range[None, :]).astype(jnp.int32)
    expert_loads = jnp.sum(onehot, axis=0).astype(jnp.int32)
    earlier = (jnp.cumsum(onehot, axis=0).astype(jnp.int32) - onehot) * onehot
    slot_ranks = jnp.sum(earlier, axis=1).astype(jnp.int32)
    holder = (TOKENS // TOK_DEV) * CAP
    token_of_pair = (jnp.arange(pair_count, dtype=jnp.int32) // TOP).astype(jnp.int32)
    table = jnp.full((EXPERTS, holder), TOKENS, jnp.int32).at[pair_ids, slot_ranks].set(token_of_pair)
    padded = jnp.concatenate([tokens, jnp.zeros((1, D), jnp.bfloat16)], axis=0)

    def one_expert(packed):
        row_index, gate_part, up_part, down_part = packed
        token_rows = padded[row_index]
        gate_value = jnp.dot(token_rows, gate_part, preferred_element_type=jnp.float32)
        up_value = jnp.dot(token_rows, up_part, preferred_element_type=jnp.float32)
        hidden = (jax.nn.silu(gate_value) * up_value).astype(jnp.bfloat16)
        result = lax.dot_general(hidden, down_part, (((1,), (1,)), ((), ())), preferred_element_type=jnp.float32)
        return result.astype(jnp.bfloat16)

    outputs = lax.map(one_expert, (table, w_gate, w_up, w_down))
    picked = outputs[pair_ids, slot_ranks].reshape(TOKENS, TOP, D)
    mixed = jnp.sum(gate_weights[:, :, None] * picked.astype(jnp.float32), axis=1)
    return mixed.astype(jnp.bfloat16), expert_loads
```

```python
import functools

import jax
import jax.numpy as jnp
from jax import lax
from jax.experimental import pallas as pl
from jax.experimental.pallas import tpu as pltpu
from jax.sharding import PartitionSpec as P

MESH = pl.DeviceIdType.MESH
BF16 = jnp.bfloat16
F32 = jnp.float32
LANES = 128
CAP = 2
GROUPS = ((0, 1), (1, 2), (3, 1))


def iota(shape, dim):
    return lax.broadcasted_iota(jnp.int32, shape, dim)


def dot(a, b):
    return jnp.dot(a, b, preferred_element_type=F32)


def dot_nt(a, b):
    return lax.dot_general(a, b, (((1,), (1,)), ((), ())), preferred_element_type=F32)


def kernel(
    ring, tokens, ids, gates, wg_hbm, wu_hbm, wd_hbm, out, loads,
    wg, wu, wd, chunk, packed, xrecv, xf, yf, yb, ra, rb, sa, sb, eo, ret,
    gsel, oparts, ksend, krecv, fsend, frecv, cnt, crecv, csum, cx,
    wsem, cs, cr, c3s, c3r, ls, lr, x1s, x1r, x2s, x2r, r1s, r1r, r2s, r2r,
    ts, tr, k3s, k3r, kfs, kfr, ns, nr, ncs, ncr,
):
    jump = ring // 4
    half = jump // 2
    slots = 2 * jump
    tok, width = tokens.shape
    qw = width // 4
    tiles = qw // LANES
    piece = 4 * CAP
    prow = slots * piece
    lanes = chunk.shape[2] - width
    meta = lanes // 2
    experts = meta // CAP
    top = ids.shape[1]
    cols = (0, qw, 2 * qw + meta, 3 * qw + meta)
    mid = 2 * qw + meta

    z, x, c = lax.axis_index("ep"), lax.axis_index("tp"), lax.axis_index("dp")
    own = (half - c) * 2 + c

    def at_z(d):
        return {"ep": lax.rem(z + d + 2 * ring, ring), "tp": x, "dp": c}

    def at_x(d):
        return {"ep": z, "tp": lax.rem(x + d + 4, 4), "dp": c}

    def out_peer(s):
        return {"ep": lax.rem(z + s // 2 - half + c + ring, ring), "tp": x, "dp": lax.rem(s, 2)}

    def in_peer(s):
        core = lax.rem(s, 2)
        return {"ep": lax.rem(z - s // 2 + half - core + ring, ring), "tp": x, "dp": core}

    def remote(src, dst, send, recv, peer):
        return pltpu.make_async_remote_copy(
            src_ref=src, dst_ref=dst, send_sem=send, recv_sem=recv, device_id=peer, device_id_type=MESH
        )

    def arrived(ref, sem):
        pltpu.make_async_copy(ref, ref, sem).wait()

    weights = [
        pltpu.make_async_copy(src, dst, wsem.at[i])
        for i, (src, dst) in enumerate(((wg_hbm, wg), (wu_hbm, wu), (wd_hbm, wd)))
    ]

    barrier = pltpu.get_barrier_semaphore()

    def greet(peer):
        pl.semaphore_signal(barrier, inc=1, device_id=peer, device_id_type=MESH)

    greet(at_z(jump))
    greet(at_z(-jump))

    def greet_local(i, carry):
        s = lax.rem(own + i, slots)
        greet(out_peer(s))
        greet(in_peer(s))
        return carry

    lax.fori_loop(1, slots, greet_local, 0)
    greet(at_x(1))
    greet(at_x(-1))
    for copy in weights:
        copy.start()

    lane = iota((tok, meta), 1)
    expert_lane = jnp.where(lane >= experts, lane - experts, lane)
    rank_lane = jnp.where(lane >= experts, 1, 0)
    hit = jnp.zeros((tok, meta), F32)
    gate = jnp.zeros((tok, meta), F32)
    for k in range(top):
        same = ids[:, k : k + 1] == expert_lane
        hit = hit + jnp.where(same, 1.0, 0.0)
        gate = gate + jnp.where(same, gates[:, k : k + 1], 0.0)
    earlier = jnp.where(iota((tok, tok), 1) < iota((tok, tok), 0), 1.0, 0.0).astype(BF16)
    rank = dot(earlier, hit.astype(BF16))
    gate = jnp.where(rank == rank_lane.astype(F32), gate, 0.0)
    gate_hi = gate.astype(BF16)
    gate_lo = (gate - gate_hi.astype(F32)).astype(BF16)
    chunk[0, :, 0 : 2 * qw] = tokens[:, 0 : 2 * qw]
    chunk[0, :, 2 * qw : mid] = gate_hi
    chunk[0, :, mid : mid + 2 * qw] = tokens[:, 2 * qw :]
    chunk[0, :, mid + 2 * qw :] = gate_lo

    pl.semaphore_wait(barrier, 2 * (slots - 1) + 4)

    jumps = [
        remote(chunk.at[0], chunk.at[1], cs.at[0], cr.at[0], at_z(jump)),
        remote(chunk.at[0], chunk.at[2], cs.at[1], cr.at[1], at_z(-jump)),
    ]
    for copy in jumps:
        copy.start()

    row = iota((prow, meta), 0)
    lane = iota((prow, meta), 1)
    row_slot = row // piece
    row_z = lax.rem(z + row_slot // 2 - half + c + ring, ring)
    row_expert = row_z * 2 + lax.rem(row_slot, 2)
    row_rank = lax.rem(row // 4, CAP)
    pick = jnp.where(row_rank * experts + row_expert == lane, 1.0, 0.0).astype(BF16)
    quarter_r = lax.rem(iota((prow, 4 * tok), 0), 4) == iota((prow, 4 * tok), 1) // tok
    quarter_c = lax.rem(iota((4 * tok, prow), 1), 4) == iota((4 * tok, prow), 0) // tok

    def pack(m):
        hi = chunk[m, :, 2 * qw : mid]
        lo = chunk[m, :, mid + 2 * qw :]
        used = jnp.where(hi.astype(F32) > 0.0, 1.0, 0.0)
        count = jnp.sum(used, axis=0, keepdims=True)
        used = used.astype(BF16)
        select = dot_nt(pick, jnp.concatenate([used] * 4, axis=0))
        select = jnp.where(quarter_r, select, 0.0).astype(BF16)
        quarters = jnp.concatenate([chunk[m, :, o : o + qw] for o in cols], axis=0)
        rows = dot(select, quarters).astype(BF16)
        packed[pl.ds(m * slots, slots)] = rows.reshape(slots, piece, qw)
        for h, part in enumerate((hi, lo)):
            mix = dot_nt(jnp.concatenate([part] * 4, axis=0), pick)
            gsel[m, pl.ds(h * 4 * tok, 4 * tok), :] = jnp.where(quarter_c, mix, 0.0).astype(BF16)
        return count

    def send_local(m):
        def body(i, carry):
            s = lax.rem(own + i, slots)
            remote(
                packed.at[m * slots + s],
                xrecv.at[0, m * slots + lax.rem(s // 2 * 2 + c, slots)],
                ls.at[m], lr.at[m], out_peer(s),
            ).start()
            return carry

        pltpu.make_async_copy(packed.at[m * slots + own], xrecv.at[0, m * slots + own], lr.at[m]).start()
        lax.fori_loop(1, slots, body, 0)

    def span(g):
        m0, nm = GROUPS[g]
        return m0 * slots, nm * slots

    def halves(g):
        s0, n = span(g)
        return pl.ds(s0, n // 2), pl.ds(s0 + n // 2, n // 2)

    def x1_copies(g):
        s0, n = span(g)
        part = xrecv.at[0, pl.ds(s0, n)]
        return [
            remote(part, xrecv.at[1, pl.ds(s0, n)], x1s.at[g, 0], x1r.at[g, 0], at_x(1)),
            remote(part, xrecv.at[3, pl.ds(s0, n)], x1s.at[g, 1], x1r.at[g, 1], at_x(-1)),
        ]

    def x2_copies(g):
        a, b = halves(g)
        return [
            remote(xrecv.at[1, a], xrecv.at[2, a], x2s.at[g, 0], x2r.at[g, 0], at_x(1)),
            remote(xrecv.at[3, b], xrecv.at[2, b], x2s.at[g, 1], x2r.at[g, 1], at_x(-1)),
        ]

    def gather_1(g):
        m0, nm = GROUPS[g]
        for m in range(m0, m0 + nm):
            arrived(xrecv.at[0, pl.ds(m * slots, slots)], lr.at[m])
        for copy in x1_copies(g):
            copy.start()

    def gather_2(g):
        for one, two in zip(x1_copies(g), x2_copies(g)):
            one.wait_recv()
            two.start()

    def ffn(g):
        s0, n = span(g)
        count = 4 * n * piece
        rows = count // 4
        for copy in x2_copies(g):
            copy.wait_recv()
        for j in range(tiles):
            arrivals = xrecv[:, pl.ds(s0, n), :, j * LANES : (j + 1) * LANES]
            xf[j, pl.ds(0, count)] = arrivals.astype(F32).reshape(count, LANES)
        full = jnp.concatenate(
            [
                xf[j, pl.ds(q, rows, stride=4), :].astype(BF16)
                for q in range(4)
                for j in range(tiles)
            ],
            axis=1,
        )
        gate_value = dot(full, wg[...])
        up_value = dot(full, wu[...])
        hidden = (gate_value / (1.0 + jnp.exp(-gate_value)) * up_value).astype(BF16)
        for q in range(4):
            terms = dot_nt(hidden, wd[pl.ds(q * qw, qw), :])
            for j in range(tiles):
                place = pl.ds(4 * s0 * piece + q, rows, stride=4)
                yf[j, place, :] = terms[:, j * LANES : (j + 1) * LANES]
        yb[1, pl.ds(s0, n)] = partial(g, 2, 0, n).astype(BF16)
        for copy in r1_copies(g):
            copy.start()

    def partial(g, column, first, number):
        s0, n = span(g)
        start = (4 * s0 + column * n + first) * piece
        parts = [yf[j, pl.ds(start, number * piece), :] for j in range(tiles)]
        return jnp.concatenate(parts, axis=1).reshape(number, piece, qw)

    def r1_copies(g):
        a, b = halves(g)
        return [
            remote(yb.at[1, a], ra.at[a], r1s.at[g, 0], r1r.at[g, 0], at_x(1)),
            remote(yb.at[1, b], rb.at[b], r1s.at[g, 1], r1r.at[g, 1], at_x(-1)),
        ]

    def r2_copies(g):
        s0, n = span(g)
        part = pl.ds(s0, n)
        return [
            remote(yb.at[2, part], sa.at[part], r2s.at[g, 0], r2r.at[g, 0], at_x(1)),
            remote(yb.at[0, part], sb.at[part], r2s.at[g, 1], r2r.at[g, 1], at_x(-1)),
        ]

    def reduce_1(g):
        s0, n = span(g)
        a, b = halves(g)
        one, two = r1_copies(g), r2_copies(g)
        yb[2, b] = partial(g, 3, n // 2, n // 2).astype(BF16)
        yb[0, a] = partial(g, 1, 0, n // 2).astype(BF16)
        one[0].wait_recv()
        yb[2, a] = (partial(g, 3, 0, n // 2) + ra[a].astype(F32)).astype(BF16)
        two[0].start()
        one[1].wait_recv()
        yb[0, b] = (partial(g, 1, n // 2, n // 2) + rb[b].astype(F32)).astype(BF16)
        two[1].start()

    def reduce_2(g):
        m0, nm = GROUPS[g]
        s0, n = span(g)
        part = pl.ds(s0, n)
        for copy in r2_copies(g):
            copy.wait_recv()
        eo[part] = (partial(g, 0, 0, n) + sa[part].astype(F32) + sb[part].astype(F32)).astype(BF16)
        for m in range(m0, m0 + nm):
            send_back(m)

    def send_back(m):
        def body(i, carry):
            s = lax.rem(own + i, slots)
            remote(
                eo.at[m * slots + s],
                ret.at[m * slots + lax.rem(s // 2 * 2 + c, slots)],
                ts.at[m], tr.at[m], in_peer(s),
            ).start()
            return carry

        pltpu.make_async_copy(eo.at[m * slots + own], ret.at[m * slots + own], tr.at[m]).start()
        lax.fori_loop(1, slots, body, 0)

    def combine(m):
        part = pl.ds(m * slots, slots)
        arrived(ret.at[part], tr.at[m])
        rows = ret[part].astype(F32).reshape(prow, qw).astype(BF16)
        both = dot(gsel[m], rows)
        quarters = both[0 : 4 * tok] + both[4 * tok :]
        return jnp.concatenate([quarters[q * tok : (q + 1) * tok] for q in range(4)], axis=1)

    def k3_copies():
        low, high = pl.ds(0, 2 * qw), pl.ds(2 * qw, 2 * qw)
        return [
            remote(ksend.at[:, low], krecv.at[:, low], k3s.at[0], k3r.at[0], at_z(-jump)),
            remote(ksend.at[:, high], krecv.at[:, high], k3s.at[1], k3r.at[1], at_z(jump)),
        ]

    def kf_copies():
        return [
            remote(fsend.at[0], frecv.at[0], kfs.at[0], kfr.at[0], at_z(-jump)),
            remote(fsend.at[1], frecv.at[1], kfs.at[1], kfr.at[1], at_z(jump)),
        ]

    count = pack(0)
    send_local(0)
    low, high = pl.ds(0, mid), pl.ds(mid, mid)
    onward = [
        remote(chunk.at[1, :, low], chunk.at[3, :, low], c3s.at[0], c3r.at[0], at_z(jump)),
        remote(chunk.at[2, :, high], chunk.at[3, :, high], c3s.at[1], c3r.at[1], at_z(-jump)),
    ]
    for first, second in zip(jumps, onward):
        first.wait_recv()
        second.start()
    count = count + pack(1)
    send_local(1)
    count = count + pack(2)
    send_local(2)
    gather_1(0)
    gather_2(0)
    gather_1(1)
    for copy in onward:
        copy.wait_recv()
    count = count + pack(3)
    send_local(3)

    cnt[...] = count

    def send_count(i, carry):
        s = lax.rem(own + i, slots)
        remote(cnt, crecv.at[lax.rem(s // 2 * 2 + c, slots)], ns, nr, out_peer(s)).start()
        return carry

    pltpu.make_async_copy(cnt, crecv.at[own], nr).start()
    lax.fori_loop(1, slots, send_count, 0)

    gather_2(1)
    for copy in weights:
        copy.wait()
    ffn(0)
    gather_1(2)
    ffn(1)
    gather_2(2)
    reduce_1(0)
    reduce_1(1)
    reduce_2(0)
    ffn(2)
    reduce_2(1)

    arrived(crecv, nr)
    csum[...] = jnp.sum(crecv[...], axis=0)
    count_1 = [
        remote(csum, cx.at[0], ncs.at[0], ncr.at[0], at_x(1)),
        remote(csum, cx.at[1], ncs.at[1], ncr.at[1], at_x(-1)),
    ]
    count_2 = remote(cx.at[0], cx.at[2], ncs.at[2], ncr.at[2], at_x(1))
    for copy in count_1:
        copy.start()

    reduce_1(2)
    count_1[0].wait_recv()
    count_2.start()
    oparts[...] = combine(0)
    reduce_2(2)
    near = [combine(1), combine(2)]
    count_1[1].wait_recv()
    count_2.wait_recv()
    total = csum[...] + cx[0] + cx[1] + cx[2]
    total = total[:, 0:experts] + total[:, experts:]
    loads[...] = total.astype(jnp.int32)

    ksend[...] = combine(3).astype(BF16)
    for copy in k3_copies():
        copy.start()
    first, second = k3_copies()
    last = kf_copies()
    first.wait_recv()
    fsend[0, :, 0 : 2 * qw] = (near[0][:, 0 : 2 * qw] + krecv[:, 0 : 2 * qw].astype(F32)).astype(BF16)
    fsend[0, :, 2 * qw :] = near[0][:, 2 * qw :].astype(BF16)
    last[0].start()
    second.wait_recv()
    fsend[1, :, 2 * qw :] = (near[1][:, 2 * qw :] + krecv[:, 2 * qw :].astype(F32)).astype(BF16)
    fsend[1, :, 0 : 2 * qw] = near[1][:, 0 : 2 * qw].astype(BF16)
    last[1].start()
    for copy in last:
        copy.wait_recv()
    out[...] = (oparts[...] + frecv[0].astype(F32) + frecv[1].astype(F32)).astype(BF16)

    sends = jumps + onward + k3_copies() + last + count_1 + [count_2]
    for g in range(len(GROUPS)):
        sends += x1_copies(g) + x2_copies(g) + r1_copies(g) + r2_copies(g)
    for copy in sends:
        copy.wait_send()
    for m in range(4):
        arrived(packed.at[pl.ds(m * slots, slots - 1)], ls.at[m])
        arrived(eo.at[pl.ds(m * slots, slots - 1)], ts.at[m])
    arrived(crecv.at[pl.ds(0, slots - 1)], ns)


def per_device(tokens, expert_ids, gate_weights, w_gate, w_up, w_down):
    tok, width = tokens.shape
    hidden = w_gate.shape[2]
    ring = lax.axis_size("ep")
    experts = ring * lax.axis_size("dp")
    slots = 2 * (ring // 4)
    qw = width // 4
    piece = 4 * CAP
    meta = CAP * experts
    prow = slots * piece
    ng = len(GROUPS)
    vmem = pltpu.VMEM
    dma = pltpu.SemaphoreType.DMA
    block = (4 * slots, piece, qw)
    scratch = [
        vmem((width, hidden), BF16), vmem((width, hidden), BF16), vmem((width, hidden), BF16),
        vmem((4, tok, width + 2 * meta), BF16),
        vmem(block, BF16),
        vmem((4, *block), BF16),
        vmem((qw // LANES, 2 * 4 * prow, LANES), F32),
        vmem((qw // LANES, 4 * 4 * prow, LANES), F32),
        vmem((3, *block), BF16),
        vmem(block, BF16), vmem(block, BF16), vmem(block, BF16), vmem(block, BF16),
        vmem(block, BF16), vmem(block, BF16),
        vmem((4, 8 * tok, prow), BF16),
        vmem((tok, width), F32),
        vmem((tok, width), BF16), vmem((tok, width), BF16),
        vmem((2, tok, width), BF16), vmem((2, tok, width), BF16),
        vmem((1, meta), F32), vmem((slots, 1, meta), F32),
        vmem((1, meta), F32), vmem((3, 1, meta), F32),
        dma((3,)), dma((2,)), dma((2,)), dma((2,)), dma((2,)),
        dma((4,)), dma((4,)),
        dma((ng, 2)), dma((ng, 2)), dma((ng, 2)), dma((ng, 2)),
        dma((ng, 2)), dma((ng, 2)), dma((ng, 2)), dma((ng, 2)),
        dma((4,)), dma((4,)), dma((2,)), dma((2,)), dma((2,)), dma((2,)),
        dma(()), dma(()), dma((3,)), dma((3,)),
    ]
    in_vmem = pl.BlockSpec(memory_space=pltpu.VMEM)
    in_any = pl.BlockSpec(memory_space=pl.ANY)
    mixed, loads = pl.pallas_call(
        functools.partial(kernel, ring),
        out_shape=(
            jax.ShapeDtypeStruct((tok, width), BF16),
            jax.ShapeDtypeStruct((1, experts), jnp.int32),
        ),
        in_specs=[in_vmem, in_vmem, in_vmem, in_any, in_any, in_any],
        out_specs=(in_vmem, in_vmem),
        scratch_shapes=scratch,
        compiler_params=pltpu.CompilerParams(
            collective_id=0, has_side_effects=True, vmem_limit_bytes=60 * 1024 * 1024
        ),
        name="routed_ffn",
    )(tokens, expert_ids, gate_weights, w_gate[0], w_up[0], w_down[0])
    return mixed, loads[0]


def solution(mesh):
    return jax.shard_map(
        per_device,
        mesh=mesh,
        in_specs=(
            P(("groups", "ep", "tp", "dp"), None),
            P(("groups", "ep", "tp", "dp"), None),
            P(("groups", "ep", "tp", "dp"), None),
            P(("ep", "dp"), None, "tp"),
            P(("ep", "dp"), None, "tp"),
            P(("ep", "dp"), None, "tp"),
        ),
        out_specs=(P(("groups", "ep", "tp", "dp"), None), P("groups")),
        check_vma=False,
    )
```

```python
import functools

import jax
import jax.numpy as jnp
from jax import lax
from jax.experimental import pallas as pl
from jax.experimental.pallas import tpu as pltpu
from jax.sharding import PartitionSpec as P

MESH = pl.DeviceIdType.MESH
BF16 = jnp.bfloat16
F32 = jnp.float32
LANES = 128
CAP = 2
N0, S0, N12, N3, S12, S3 = range(6)
GROUPS = ((1, 0, 1), (0, 0, 1), (1, 1, 2), (1, 3, 1), (0, 1, 2), (0, 3, 1))
DIRECT = (N0, S0, N3, S3)


def iota(shape, dim):
    return lax.broadcasted_iota(jnp.int32, shape, dim)


def dot(a, b):
    return jnp.dot(a, b, preferred_element_type=F32)


def dot_nt(a, b):
    return lax.dot_general(a, b, (((1,), (1,)), ((), ())), preferred_element_type=F32)


def kernel(
    ring, tokens_hbm, ids_hbm, gates_hbm, wg_hbm, wu_hbm, wd_hbm, out, loads,
    tokens, ids, gates, wg, wu, wd, chunk, packed, xrecv, xf, yf, yb, ra, rb, sa, sb, eo, ret,
    gsel, oparts, ksend, krecv, fsend, frecv, cnt, crecv, csum, cx,
    wsem, isem, cs, cr, ls, lr, x1s, x1r, x2s, x2r, r1s, r1r, r2s, r2r,
    ts, tr, k3s, k3r, kfs, kfr, ns, nr, ncs, ncr,
):
    jump = ring // 4
    half = jump // 2
    slots = 2 * jump
    tok, width = tokens.shape
    qw = width // 4
    tiles = qw // LANES
    piece = 4 * CAP
    prow = slots * piece
    lanes = chunk.shape[2] - width
    meta = lanes // 2
    experts = meta // CAP
    top = ids.shape[0]
    cols = (0, qw, 2 * qw + meta, 3 * qw + meta)
    mid = 2 * qw + meta

    z, x, c = lax.axis_index("ep"), lax.axis_index("tp"), lax.axis_index("dp")
    own = (half - c) * 2 + c

    def at_z(d):
        return {"ep": lax.rem(z + d + 2 * ring, ring), "tp": x, "dp": c}

    def at_x(d):
        return {"ep": z, "tp": lax.rem(x + d + 4, 4), "dp": c}

    def out_peer(s):
        return {"ep": lax.rem(z + s // 2 - half + c + ring, ring), "tp": x, "dp": lax.rem(s, 2)}

    def in_peer(s):
        core = lax.rem(s, 2)
        return {"ep": lax.rem(z - s // 2 + half - core + ring, ring), "tp": x, "dp": core}

    def remote(src, dst, send, recv, peer):
        return pltpu.make_async_remote_copy(
            src_ref=src, dst_ref=dst, send_sem=send, recv_sem=recv, device_id=peer, device_id_type=MESH
        )

    def arrived(ref, sem):
        pltpu.make_async_copy(ref, ref, sem).wait()

    weights = [
        pltpu.make_async_copy(src, dst, wsem.at[i])
        for i, (src, dst) in enumerate(((wg_hbm, wg), (wu_hbm, wu), (wd_hbm, wd)))
    ]

    inputs = [
        pltpu.make_async_copy(src, dst, isem.at[i])
        for i, (src, dst) in enumerate(((ids_hbm, ids), (gates_hbm, gates), (tokens_hbm, tokens)))
    ]
    for copy in inputs:
        copy.start()

    barrier = pltpu.get_barrier_semaphore()

    def greet(peer):
        pl.semaphore_signal(barrier, inc=1, device_id=peer, device_id_type=MESH)

    greet(at_z(jump))
    greet(at_z(-jump))

    def greet_local(i, carry):
        s = lax.rem(own + i, slots)
        greet(out_peer(s))
        greet(in_peer(s))
        return carry

    lax.fori_loop(1, slots, greet_local, 0)
    greet(at_x(1))
    greet(at_x(-1))
    greet(at_x(2))
    for copy in weights:
        copy.start()

    for copy in inputs:
        copy.wait()

    line = iota((meta, tok), 0)
    line_expert = jnp.where(line >= experts, line - experts, line)
    line_rank = jnp.where(line >= experts, 1.0, 0.0)
    hit = jnp.zeros((meta, tok), F32)
    gate = jnp.zeros((meta, tok), F32)
    for k in range(top):
        same = ids[k : k + 1, :] == line_expert
        hit = hit + jnp.where(same, 1.0, 0.0)
        gate = gate + jnp.where(same, gates[k : k + 1, :], 0.0)
    row, column = iota((tok, tok), 0), iota((tok, tok), 1)
    rank = dot(hit.astype(BF16), jnp.where(row < column, 1.0, 0.0).astype(BF16))
    gate = jnp.where(rank == line_rank, gate, 0.0)
    gate_hi = gate.astype(BF16)
    gate_lo = (gate - gate_hi.astype(F32)).astype(BF16)
    unit = jnp.where(row == column, 1.0, 0.0).astype(BF16)
    gate_hi = dot_nt(unit, gate_hi).astype(BF16)
    gate_lo = dot_nt(unit, gate_lo).astype(BF16)
    chunk[0, :, 0 : 2 * qw] = tokens[:, 0 : 2 * qw]
    chunk[0, :, 2 * qw : mid] = gate_hi
    chunk[0, :, mid : mid + 2 * qw] = tokens[:, 2 * qw :]
    chunk[0, :, mid + 2 * qw :] = gate_lo

    pl.semaphore_wait(barrier, 2 * (slots - 1) + 5)

    low, high = pl.ds(0, mid), pl.ds(mid, mid)

    def jump_copy(i, part, source, target, where):
        return remote(
            chunk.at[source, :, part], chunk.at[target, :, part], cs.at[i], cr.at[i], at_z(where)
        )

    jumps = [
        jump_copy(0, low, 0, 1, jump),
        jump_copy(1, high, 0, 2, -jump),
        jump_copy(2, high, 0, 1, jump),
        jump_copy(3, low, 0, 2, -jump),
    ]
    onward = [jump_copy(4, low, 1, 3, jump), jump_copy(5, high, 2, 3, -jump)]
    for copy in jumps:
        copy.start()

    row = iota((prow, meta), 0)
    lane = iota((prow, meta), 1)
    row_slot = row // piece
    row_z = lax.rem(z + row_slot // 2 - half + c + ring, ring)
    row_expert = row_z * 2 + lax.rem(row_slot, 2)
    row_rank = lax.rem(row // 4, CAP)
    pick = jnp.where(row_rank * experts + row_expert == lane, 1.0, 0.0).astype(BF16)
    quarter_r = lax.rem(iota((prow, 4 * tok), 0), 4) == iota((prow, 4 * tok), 1) // tok
    quarter_c = lax.rem(iota((4 * tok, prow), 1), 4) == iota((4 * tok, prow), 0) // tok

    def pack(m):
        hi = chunk[m, :, 2 * qw : mid]
        lo = chunk[m, :, mid + 2 * qw :]
        used = jnp.where(hi.astype(F32) > 0.0, 1.0, 0.0)
        count = jnp.sum(used, axis=0, keepdims=True)
        used = used.astype(BF16)
        select = dot_nt(pick, jnp.concatenate([used] * 4, axis=0))
        select = jnp.where(quarter_r, select, 0.0).astype(BF16)
        quarters = jnp.concatenate([chunk[m, :, o : o + qw] for o in cols], axis=0)
        rows = dot(select, quarters).astype(BF16)
        packed[pl.ds(m * slots, slots)] = rows.reshape(slots, piece, qw)
        for h, part in enumerate((hi, lo)):
            mix = dot_nt(jnp.concatenate([part] * 4, axis=0), pick)
            gsel[m, pl.ds(h * 4 * tok, 4 * tok), :] = jnp.where(quarter_c, mix, 0.0).astype(BF16)
        return count

    def send_local(m):
        def body(i, carry):
            s = lax.rem(own + i, slots)
            remote(
                packed.at[m * slots + s],
                xrecv.at[0, (c * 4 + m) * jump + s // 2],
                ls.at[m], lr.at[c * 4 + m], out_peer(s),
            ).start()
            return carry

        here = xrecv.at[0, (c * 4 + m) * jump + own // 2]
        pltpu.make_async_copy(packed.at[m * slots + own], here, lr.at[c * 4 + m]).start()
        lax.fori_loop(1, slots, body, 0)

    def span(g):
        core, m0, nm = GROUPS[g]
        return (core * 4 + m0) * jump, nm * jump

    def halves(g):
        s0, n = span(g)
        return pl.ds(s0, n // 2), pl.ds(s0 + n // 2, n // 2)

    def x1_copies(g):
        s0, n = span(g)
        part = xrecv.at[0, pl.ds(s0, n)]
        if g in DIRECT:
            across = [remote(part, xrecv.at[2, pl.ds(s0, n)], x2s.at[g, 0], x2r.at[g, 0], at_x(2))]
        else:
            across = []
        return across + [
            remote(part, xrecv.at[1, pl.ds(s0, n)], x1s.at[g, 0], x1r.at[g, 0], at_x(1)),
            remote(part, xrecv.at[3, pl.ds(s0, n)], x1s.at[g, 1], x1r.at[g, 1], at_x(-1)),
        ]

    def x2_copies(g):
        a, b = halves(g)
        return [
            remote(xrecv.at[1, a], xrecv.at[2, a], x2s.at[g, 0], x2r.at[g, 0], at_x(1)),
            remote(xrecv.at[3, b], xrecv.at[2, b], x2s.at[g, 1], x2r.at[g, 1], at_x(-1)),
        ]

    def gather_1(g):
        core, m0, nm = GROUPS[g]
        for n in range(core * 4 + m0, core * 4 + m0 + nm):
            arrived(xrecv.at[0, pl.ds(n * jump, jump)], lr.at[n])
        for copy in x1_copies(g):
            copy.start()

    def gather_2(g):
        for one, two in zip(x1_copies(g), x2_copies(g)):
            one.wait_recv()
            two.start()

    def ffn(g):
        s0, n = span(g)
        count = 4 * n * piece
        rows = count // 4
        for copy in x1_copies(g) if g in DIRECT else x2_copies(g):
            copy.wait_recv()
        for j in range(tiles):
            arrivals = xrecv[:, pl.ds(s0, n), :, j * LANES : (j + 1) * LANES]
            xf[j, pl.ds(0, count)] = arrivals.astype(F32).reshape(count, LANES)
        full = jnp.concatenate(
            [
                xf[j, pl.ds(q, rows, stride=4), :].astype(BF16)
                for q in range(4)
                for j in range(tiles)
            ],
            axis=1,
        )
        gate_value = dot(full, wg[...])
        up_value = dot(full, wu[...])
        hidden = (gate_value / (1.0 + jnp.exp(-gate_value)) * up_value).astype(BF16)
        for q in range(4):
            terms = dot_nt(hidden, wd[pl.ds(q * qw, qw), :])
            for j in range(tiles):
                place = pl.ds(4 * s0 * piece + q, rows, stride=4)
                yf[j, place, :] = terms[:, j * LANES : (j + 1) * LANES]
        part = pl.ds(s0, n)
        yb[1, part] = partial(g, 2, 0, n).astype(BF16)
        for copy in r1_copies(g):
            copy.start()
        if g in DIRECT:
            yb[2, part] = partial(g, 3, 0, n).astype(BF16)
            yb[0, part] = partial(g, 1, 0, n).astype(BF16)
            for copy in r2_copies(g):
                copy.start()

    def partial(g, column, first, number):
        s0, n = span(g)
        start = (4 * s0 + column * n + first) * piece
        parts = [yf[j, pl.ds(start, number * piece), :] for j in range(tiles)]
        return jnp.concatenate(parts, axis=1).reshape(number, piece, qw)

    def r1_copies(g):
        a, b = halves(g)
        if g in DIRECT:
            s0, n = span(g)
            part = pl.ds(s0, n)
            return [remote(yb.at[1, part], ra.at[part], r1s.at[g, 0], r1r.at[g, 0], at_x(2))]
        return [
            remote(yb.at[1, a], ra.at[a], r1s.at[g, 0], r1r.at[g, 0], at_x(1)),
            remote(yb.at[1, b], rb.at[b], r1s.at[g, 1], r1r.at[g, 1], at_x(-1)),
        ]

    def r2_copies(g):
        s0, n = span(g)
        part = pl.ds(s0, n)
        return [
            remote(yb.at[2, part], sa.at[part], r2s.at[g, 0], r2r.at[g, 0], at_x(1)),
            remote(yb.at[0, part], sb.at[part], r2s.at[g, 1], r2r.at[g, 1], at_x(-1)),
        ]

    def reduce_1(g):
        s0, n = span(g)
        a, b = halves(g)
        one, two = r1_copies(g), r2_copies(g)
        yb[2, b] = partial(g, 3, n // 2, n // 2).astype(BF16)
        yb[0, a] = partial(g, 1, 0, n // 2).astype(BF16)
        one[0].wait_recv()
        yb[2, a] = (partial(g, 3, 0, n // 2) + ra[a].astype(F32)).astype(BF16)
        two[0].start()
        one[1].wait_recv()
        yb[0, b] = (partial(g, 1, n // 2, n // 2) + rb[b].astype(F32)).astype(BF16)
        two[1].start()

    def reduce_2(g):
        core, m0, nm = GROUPS[g]
        s0, n = span(g)
        part = pl.ds(s0, n)
        for copy in r2_copies(g):
            copy.wait_recv()
        total = partial(g, 0, 0, n) + sa[part].astype(F32) + sb[part].astype(F32)
        if g in DIRECT:
            for copy in r1_copies(g):
                copy.wait_recv()
            total = total + ra[part].astype(F32)
        eo[part] = total.astype(BF16)
        for m in range(m0, m0 + nm):
            send_back(core, m)

    def send_back(core, m):
        def peer(i):
            n = lax.rem(half - core + i, jump)
            source = eo.at[(core * 4 + m) * jump + n]
            place = ret.at[m * slots + n * 2 + c]
            where = {"ep": lax.rem(z - n + half - core + ring, ring), "tp": x, "dp": core}
            return source, place, where

        def body(i, carry):
            source, place, where = peer(i)
            remote(source, place, ts.at[m], tr.at[m], where).start()
            return carry

        source, place, where = peer(0)

        @pl.when(c == core)
        def _():
            pltpu.make_async_copy(source, place, tr.at[m]).start()

        @pl.when(c != core)
        def _():
            remote(source, place, ts.at[m], tr.at[m], where).start()

        lax.fori_loop(1, jump, body, 0)

    def combine(m):
        part = pl.ds(m * slots, slots)
        arrived(ret.at[part], tr.at[m])
        rows = ret[part].astype(F32).reshape(prow, qw).astype(BF16)
        both = dot(gsel[m], rows)
        quarters = both[0 : 4 * tok] + both[4 * tok :]
        return jnp.concatenate([quarters[q * tok : (q + 1) * tok] for q in range(4)], axis=1)

    left, right = pl.ds(0, 2 * qw), pl.ds(2 * qw, 2 * qw)

    def k3_copies():
        return [
            remote(ksend.at[:, left], krecv.at[:, left], k3s.at[0], k3r.at[0], at_z(-jump)),
            remote(ksend.at[:, right], krecv.at[:, right], k3s.at[1], k3r.at[1], at_z(jump)),
        ]

    def kf_copy(i, number, part, where):
        return remote(
            fsend.at[number, :, part], frecv.at[number, :, part], kfs.at[i], kfr.at[i], at_z(where)
        )

    kf_copies = [
        kf_copy(0, 0, right, -jump),
        kf_copy(1, 1, left, jump),
        kf_copy(2, 0, left, -jump),
        kf_copy(3, 1, right, jump),
    ]

    count = pack(0)
    send_local(0)
    for first, second in zip(jumps, onward):
        first.wait_recv()
        second.start()
    jumps[2].wait_recv()
    count = count + pack(1)
    send_local(1)
    jumps[3].wait_recv()
    count = count + pack(2)
    send_local(2)
    gather_1(N0)
    gather_1(S0)
    gather_1(N12)
    for copy in onward:
        copy.wait_recv()
    count = count + pack(3)
    send_local(3)

    cnt[...] = count

    def send_count(i, carry):
        s = lax.rem(own + i, slots)
        remote(cnt, crecv.at[lax.rem(s // 2 * 2 + c, slots)], ns, nr, out_peer(s)).start()
        return carry

    pltpu.make_async_copy(cnt, crecv.at[own], nr).start()
    lax.fori_loop(1, slots, send_count, 0)

    for copy in weights:
        copy.wait()
    ffn(N0)
    ffn(S0)
    gather_2(N12)
    gather_1(N3)
    gather_1(S12)
    gather_1(S3)
    ffn(N12)
    ffn(N3)
    reduce_2(N0)
    reduce_2(S0)
    gather_2(S12)
    reduce_1(N12)
    ffn(S3)
    ffn(S12)
    reduce_2(N3)
    reduce_2(N12)
    arrived(crecv, nr)
    csum[...] = jnp.sum(crecv[...], axis=0)
    count_1 = [
        remote(csum, cx.at[0], ncs.at[0], ncr.at[0], at_x(1)),
        remote(csum, cx.at[1], ncs.at[1], ncr.at[1], at_x(-1)),
        remote(csum, cx.at[2], ncs.at[2], ncr.at[2], at_x(2)),
    ]
    for copy in count_1:
        copy.start()
    reduce_2(S3)
    reduce_1(S12)
    oparts[...] = combine(0)

    ksend[...] = combine(3).astype(BF16)
    for copy in k3_copies():
        copy.start()
    reduce_2(S12)
    near = [combine(1), combine(2)]
    fsend[0, :, 2 * qw :] = near[0][:, 2 * qw :].astype(BF16)
    kf_copies[0].start()
    fsend[1, :, 0 : 2 * qw] = near[1][:, 0 : 2 * qw].astype(BF16)
    kf_copies[1].start()
    for copy in count_1:
        copy.wait_recv()
    total = csum[...] + cx[0] + cx[1] + cx[2]
    total = total[:, 0:experts] + total[:, experts:]
    loads[...] = total.astype(jnp.int32)
    k3 = k3_copies()
    k3[0].wait_recv()
    fsend[0, :, 0 : 2 * qw] = (near[0][:, 0 : 2 * qw] + krecv[:, 0 : 2 * qw].astype(F32)).astype(BF16)
    kf_copies[2].start()
    k3[1].wait_recv()
    fsend[1, :, 2 * qw :] = (near[1][:, 2 * qw :] + krecv[:, 2 * qw :].astype(F32)).astype(BF16)
    kf_copies[3].start()
    for copy in kf_copies:
        copy.wait_recv()
    out[...] = (oparts[...] + frecv[0].astype(F32) + frecv[1].astype(F32)).astype(BF16)

    sends = jumps + onward + k3_copies() + kf_copies + count_1
    for g in range(len(GROUPS)):
        sends += x1_copies(g) + r1_copies(g) + r2_copies(g)
        if g not in DIRECT:
            sends += x2_copies(g)
    for copy in sends:
        copy.wait_send()
    for m in range(4):
        arrived(packed.at[pl.ds(m * slots, slots - 1)], ls.at[m])
        arrived(eo.at[pl.ds(m * slots, slots - 1)], ts.at[m])
    arrived(crecv.at[pl.ds(0, slots - 1)], ns)


def per_device(tokens, expert_ids, gate_weights, w_gate, w_up, w_down):
    tok, width = tokens.shape
    hidden = w_gate.shape[2]
    ring = lax.axis_size("ep")
    experts = ring * lax.axis_size("dp")
    slots = 2 * (ring // 4)
    qw = width // 4
    piece = 4 * CAP
    meta = CAP * experts
    prow = slots * piece
    ng = len(GROUPS)
    vmem = pltpu.VMEM
    dma = pltpu.SemaphoreType.DMA
    block = (4 * slots, piece, qw)
    scratch = [
        vmem((tok, width), BF16), vmem(expert_ids.shape[::-1], jnp.int32), vmem(gate_weights.shape[::-1], F32),
        vmem((width, hidden), BF16), vmem((width, hidden), BF16), vmem((width, hidden), BF16),
        vmem((4, tok, width + 2 * meta), BF16),
        vmem(block, BF16),
        vmem((4, *block), BF16),
        vmem((qw // LANES, 4 * prow, LANES), F32),
        vmem((qw // LANES, 4 * 4 * prow, LANES), F32),
        vmem((3, *block), BF16),
        vmem(block, BF16), vmem(block, BF16), vmem(block, BF16), vmem(block, BF16),
        vmem(block, BF16), vmem(block, BF16),
        vmem((4, 8 * tok, prow), BF16),
        vmem((tok, width), F32),
        vmem((tok, width), BF16), vmem((tok, width), BF16),
        vmem((2, tok, width), BF16), vmem((2, tok, width), BF16),
        vmem((1, meta), F32), vmem((slots, 1, meta), F32),
        vmem((1, meta), F32), vmem((3, 1, meta), F32),
        dma((3,)), dma((3,)), dma((6,)), dma((6,)), dma((4,)), dma((8,)),
        dma((ng, 2)), dma((ng, 2)), dma((ng, 2)), dma((ng, 2)),
        dma((ng, 2)), dma((ng, 2)), dma((ng, 2)), dma((ng, 2)),
        dma((4,)), dma((4,)), dma((2,)), dma((2,)), dma((4,)), dma((4,)),
        dma(()), dma(()), dma((3,)), dma((3,)),
    ]
    in_vmem = pl.BlockSpec(memory_space=pltpu.VMEM)
    in_any = pl.BlockSpec(memory_space=pl.ANY)
    mixed, loads = pl.pallas_call(
        functools.partial(kernel, ring),
        out_shape=(
            jax.ShapeDtypeStruct((tok, width), BF16),
            jax.ShapeDtypeStruct((1, experts), jnp.int32),
        ),
        in_specs=[in_any] * 6,
        out_specs=(in_vmem, in_vmem),
        scratch_shapes=scratch,
        compiler_params=pltpu.CompilerParams(
            collective_id=0, has_side_effects=True, vmem_limit_bytes=60 * 1024 * 1024
        ),
        name="routed_ffn",
    )(tokens, expert_ids.T, gate_weights.T, w_gate[0], w_up[0], w_down[0])
    return mixed, loads[0]


def solution(mesh):
    return jax.shard_map(
        per_device,
        mesh=mesh,
        in_specs=(
            P(("groups", "ep", "tp", "dp"), None),
            P(("groups", "ep", "tp", "dp"), None),
            P(("groups", "ep", "tp", "dp"), None),
            P(("ep", "dp"), None, "tp"),
            P(("ep", "dp"), None, "tp"),
            P(("ep", "dp"), None, "tp"),
        ),
        out_specs=(P(("groups", "ep", "tp", "dp"), None), P("groups")),
        check_vma=False,
    )
```

```python
import functools

import jax
import jax.numpy as jnp
from jax import lax
from jax.experimental import pallas as pl
from jax.experimental.pallas import tpu as pltpu
from jax.sharding import PartitionSpec as P

MESH = pl.DeviceIdType.MESH
BF16 = jnp.bfloat16
F32 = jnp.float32
LANES = 128
CAP = 2
N0, S0, N12, N3, S12, S3 = range(6)
GROUPS = ((1, 0, 1), (0, 0, 1), (1, 1, 2), (1, 3, 1), (0, 1, 2), (0, 3, 1))
DIRECT = (N0, S0, N3, S3)


def iota(shape, dim):
    return lax.broadcasted_iota(jnp.int32, shape, dim)


def dot(a, b):
    return jnp.dot(a, b, preferred_element_type=F32)


def dot_nt(a, b):
    return lax.dot_general(a, b, (((1,), (1,)), ((), ())), preferred_element_type=F32)


def kernel(
    ring, tokens_hbm, ids_hbm, gates_hbm, wg_hbm, wu_hbm, wd_hbm, out, loads,
    tokens, ids, gates, wg, wu, wd, chunk, packed, xrecv, xf, yf, yb, ra, rb, sa, sb, eo, ret,
    gsel, oparts, ksend, krecv, fsend, frecv, cnt, crecv, csum, cx,
    wsem, isem, cs, cr, ls, lr, x1s, x1r, x2s, x2r, r1s, r1r, r2s, r2r,
    ts, tr, k3s, k3r, kfs, kfr, ns, nr, ncs, ncr,
):
    jump = ring // 4
    half = jump // 2
    slots = 2 * jump
    tok, width = tokens.shape
    qw = width // 4
    tiles = qw // LANES
    piece = 4 * CAP
    prow = slots * piece
    lanes = chunk.shape[2] - width
    meta = lanes // 2
    experts = meta // CAP
    top = ids.shape[0]
    cols = (0, qw, 2 * qw + meta, 3 * qw + meta)
    mid = 2 * qw + meta

    z, x, c = lax.axis_index("ep"), lax.axis_index("tp"), lax.axis_index("dp")
    own = (half - c) * 2 + c

    def at_z(d):
        return {"ep": lax.rem(z + d + 2 * ring, ring), "tp": x, "dp": c}

    def at_x(d):
        return {"ep": z, "tp": lax.rem(x + d + 4, 4), "dp": c}

    def out_peer(s):
        return {"ep": lax.rem(z + s // 2 - half + c + ring, ring), "tp": x, "dp": lax.rem(s, 2)}

    def in_peer(s):
        core = lax.rem(s, 2)
        return {"ep": lax.rem(z - s // 2 + half - core + ring, ring), "tp": x, "dp": core}

    def remote(src, dst, send, recv, peer):
        return pltpu.make_async_remote_copy(
            src_ref=src, dst_ref=dst, send_sem=send, recv_sem=recv, device_id=peer, device_id_type=MESH
        )

    def arrived(ref, sem):
        pltpu.make_async_copy(ref, ref, sem).wait()

    weights = [
        pltpu.make_async_copy(src, dst, wsem.at[i])
        for i, (src, dst) in enumerate(((wg_hbm, wg), (wu_hbm, wu), (wd_hbm, wd)))
    ]

    inputs = [
        pltpu.make_async_copy(src, dst, isem.at[i])
        for i, (src, dst) in enumerate(((ids_hbm, ids), (gates_hbm, gates), (tokens_hbm, tokens)))
    ]
    for copy in inputs:
        copy.start()

    barrier = pltpu.get_barrier_semaphore()

    def greet(peer):
        pl.semaphore_signal(barrier, inc=1, device_id=peer, device_id_type=MESH)

    greet(at_z(jump))
    greet(at_z(-jump))
    for d in (1, -1, 2):
        greet(at_x(d))
    greet({"ep": z, "tp": x, "dp": 1 - c})
    for d in range(1, half):
        for step in (d, -d):
            for core in range(2):
                greet({"ep": lax.rem(z + step + ring, ring), "tp": x, "dp": core})
    greet({"ep": lax.rem(z + half, ring), "tp": x, "dp": 0})
    greet({"ep": lax.rem(z - half + ring, ring), "tp": x, "dp": 1})
    greet({"ep": lax.rem(z + (2 * c - 1) * half + ring, ring), "tp": x, "dp": c})
    for copy in weights:
        copy.start()

    for copy in inputs:
        copy.wait()

    line = iota((meta, tok), 0)
    line_expert = jnp.where(line >= experts, line - experts, line)
    line_rank = jnp.where(line >= experts, 1.0, 0.0)
    hit = jnp.zeros((meta, tok), F32)
    gate = jnp.zeros((meta, tok), F32)
    for k in range(top):
        same = ids[k : k + 1, :] == line_expert
        hit = hit + jnp.where(same, 1.0, 0.0)
        gate = gate + jnp.where(same, gates[k : k + 1, :], 0.0)
    row, column = iota((tok, tok), 0), iota((tok, tok), 1)
    rank = dot(hit.astype(BF16), jnp.where(row < column, 1.0, 0.0).astype(BF16))
    gate = jnp.where(rank == line_rank, gate, 0.0)
    gate_hi = gate.astype(BF16)
    gate_lo = (gate - gate_hi.astype(F32)).astype(BF16)
    unit = jnp.where(row == column, 1.0, 0.0).astype(BF16)
    gate_hi = dot_nt(unit, gate_hi).astype(BF16)
    gate_lo = dot_nt(unit, gate_lo).astype(BF16)
    chunk[0, :, 0 : 2 * qw] = tokens[:, 0 : 2 * qw]
    chunk[0, :, 2 * qw : mid] = gate_hi
    chunk[0, :, mid : mid + 2 * qw] = tokens[:, 2 * qw :]
    chunk[0, :, mid + 2 * qw :] = gate_lo

    pl.semaphore_wait(barrier, 4 * half + 5)

    low, high = pl.ds(0, mid), pl.ds(mid, mid)

    def jump_copy(i, part, source, target, where):
        return remote(
            chunk.at[source, :, part], chunk.at[target, :, part], cs.at[i], cr.at[i], at_z(where)
        )

    jumps = [
        jump_copy(0, low, 0, 1, jump),
        jump_copy(1, high, 0, 2, -jump),
        jump_copy(2, high, 0, 1, jump),
        jump_copy(3, low, 0, 2, -jump),
    ]
    onward = [jump_copy(4, low, 1, 3, jump), jump_copy(5, high, 2, 3, -jump)]
    for copy in jumps:
        copy.start()

    row = iota((prow, meta), 0)
    lane = iota((prow, meta), 1)
    row_slot = row // piece
    row_z = lax.rem(z + row_slot // 2 - half + c + ring, ring)
    row_expert = row_z * 2 + lax.rem(row_slot, 2)
    row_rank = lax.rem(row // 4, CAP)
    pick = jnp.where(row_rank * experts + row_expert == lane, 1.0, 0.0).astype(BF16)
    quarter_r = lax.rem(iota((prow, 4 * tok), 0), 4) == iota((prow, 4 * tok), 1) // tok
    quarter_c = lax.rem(iota((4 * tok, prow), 1), 4) == iota((4 * tok, prow), 0) // tok

    def pack(m):
        hi = chunk[m, :, 2 * qw : mid]
        lo = chunk[m, :, mid + 2 * qw :]
        used = jnp.where(hi.astype(F32) > 0.0, 1.0, 0.0)
        count = jnp.sum(used, axis=0, keepdims=True)
        used = used.astype(BF16)
        select = dot_nt(pick, jnp.concatenate([used] * 4, axis=0))
        select = jnp.where(quarter_r, select, 0.0).astype(BF16)
        quarters = jnp.concatenate([chunk[m, :, o : o + qw] for o in cols], axis=0)
        rows = dot(select, quarters).astype(BF16)
        packed[pl.ds(m * slots, slots)] = rows.reshape(slots, piece, qw)
        for h, part in enumerate((hi, lo)):
            mix = dot_nt(jnp.concatenate([part] * 4, axis=0), pick)
            gsel[m, pl.ds(h * 4 * tok, 4 * tok), :] = jnp.where(quarter_c, mix, 0.0).astype(BF16)
        return count

    def send_local(m):
        def body(i, carry):
            s = lax.rem(own + i, slots)
            remote(
                packed.at[m * slots + s],
                xrecv.at[0, (c * 4 + m) * jump + s // 2],
                ls.at[m], lr.at[c * 4 + m], out_peer(s),
            ).start()
            return carry

        here = xrecv.at[0, (c * 4 + m) * jump + own // 2]
        pltpu.make_async_copy(packed.at[m * slots + own], here, lr.at[c * 4 + m]).start()
        lax.fori_loop(1, slots, body, 0, unroll=True)

    def span(g):
        core, m0, nm = GROUPS[g]
        return (core * 4 + m0) * jump, nm * jump

    def halves(g):
        s0, n = span(g)
        return pl.ds(s0, n // 2), pl.ds(s0 + n // 2, n // 2)

    def x1_copies(g):
        s0, n = span(g)
        part = xrecv.at[0, pl.ds(s0, n)]
        if g in DIRECT:
            across = [remote(part, xrecv.at[2, pl.ds(s0, n)], x2s.at[g, 0], x2r.at[g, 0], at_x(2))]
        else:
            across = []
        return across + [
            remote(part, xrecv.at[1, pl.ds(s0, n)], x1s.at[g, 0], x1r.at[g, 0], at_x(1)),
            remote(part, xrecv.at[3, pl.ds(s0, n)], x1s.at[g, 1], x1r.at[g, 1], at_x(-1)),
        ]

    def x2_copies(g):
        a, b = halves(g)
        return [
            remote(xrecv.at[1, a], xrecv.at[2, a], x2s.at[g, 0], x2r.at[g, 0], at_x(1)),
            remote(xrecv.at[3, b], xrecv.at[2, b], x2s.at[g, 1], x2r.at[g, 1], at_x(-1)),
        ]

    def gather_1(g):
        core, m0, nm = GROUPS[g]
        for n in range(core * 4 + m0, core * 4 + m0 + nm):
            arrived(xrecv.at[0, pl.ds(n * jump, jump)], lr.at[n])
        for copy in x1_copies(g):
            copy.start()

    def gather_2(g):
        for one, two in zip(x1_copies(g), x2_copies(g)):
            one.wait_recv()
            two.start()

    def ffn(g):
        s0, n = span(g)
        count = 4 * n * piece
        rows = count // 4
        for copy in x1_copies(g) if g in DIRECT else x2_copies(g):
            copy.wait_recv()
        for j in range(tiles):
            arrivals = xrecv[:, pl.ds(s0, n), :, j * LANES : (j + 1) * LANES]
            xf[j, pl.ds(0, count)] = arrivals.astype(F32).reshape(count, LANES)
        full = jnp.concatenate(
            [
                xf[j, pl.ds(q, rows, stride=4), :].astype(BF16)
                for q in range(4)
                for j in range(tiles)
            ],
            axis=1,
        )
        gate_value = dot(full, wg[...])
        up_value = dot(full, wu[...])
        hidden = (gate_value / (1.0 + jnp.exp(-gate_value)) * up_value).astype(BF16)
        for q in range(4):
            terms = dot_nt(hidden, wd[pl.ds(q * qw, qw), :])
            for j in range(tiles):
                place = pl.ds(4 * s0 * piece + q, rows, stride=4)
                yf[j, place, :] = terms[:, j * LANES : (j + 1) * LANES]
        if g not in (N0, S0):
            spread(g)

    def spread(g):
        s0, n = span(g)
        part = pl.ds(s0, n)
        yb[1, part] = partial(g, 2, 0, n).astype(BF16)
        for copy in r1_copies(g):
            copy.start()
        if g in DIRECT:
            yb[2, part] = partial(g, 3, 0, n).astype(BF16)
            yb[0, part] = partial(g, 1, 0, n).astype(BF16)
            for copy in r2_copies(g):
                copy.start()

    def partial(g, column, first, number):
        s0, n = span(g)
        start = (4 * s0 + column * n + first) * piece
        parts = [yf[j, pl.ds(start, number * piece), :] for j in range(tiles)]
        return jnp.concatenate(parts, axis=1).reshape(number, piece, qw)

    def r1_copies(g):
        a, b = halves(g)
        if g in DIRECT:
            s0, n = span(g)
            part = pl.ds(s0, n)
            return [remote(yb.at[1, part], ra.at[part], r1s.at[g, 0], r1r.at[g, 0], at_x(2))]
        return [
            remote(yb.at[1, a], ra.at[a], r1s.at[g, 0], r1r.at[g, 0], at_x(1)),
            remote(yb.at[1, b], rb.at[b], r1s.at[g, 1], r1r.at[g, 1], at_x(-1)),
        ]

    def r2_copies(g):
        s0, n = span(g)
        part = pl.ds(s0, n)
        return [
            remote(yb.at[2, part], sa.at[part], r2s.at[g, 0], r2r.at[g, 0], at_x(1)),
            remote(yb.at[0, part], sb.at[part], r2s.at[g, 1], r2r.at[g, 1], at_x(-1)),
        ]

    def reduce_1(g):
        s0, n = span(g)
        a, b = halves(g)
        one, two = r1_copies(g), r2_copies(g)
        yb[2, b] = partial(g, 3, n // 2, n // 2).astype(BF16)
        yb[0, a] = partial(g, 1, 0, n // 2).astype(BF16)
        one[0].wait_recv()
        yb[2, a] = (partial(g, 3, 0, n // 2) + ra[a].astype(F32)).astype(BF16)
        two[0].start()
        one[1].wait_recv()
        yb[0, b] = (partial(g, 1, n // 2, n // 2) + rb[b].astype(F32)).astype(BF16)
        two[1].start()

    def reduce_2(g):
        core, m0, nm = GROUPS[g]
        s0, n = span(g)
        part = pl.ds(s0, n)
        for copy in r2_copies(g):
            copy.wait_recv()
        total = partial(g, 0, 0, n) + sa[part].astype(F32) + sb[part].astype(F32)
        if g in DIRECT:
            for copy in r1_copies(g):
                copy.wait_recv()
            total = total + ra[part].astype(F32)
        eo[part] = total.astype(BF16)
        for m in range(m0, m0 + nm):
            send_back(core, m)

    def send_back(core, m):
        def peer(i):
            n = lax.rem(half - core + i, jump)
            source = eo.at[(core * 4 + m) * jump + n]
            place = ret.at[m * slots + n * 2 + c]
            where = {"ep": lax.rem(z - n + half - core + ring, ring), "tp": x, "dp": core}
            return source, place, where

        def body(i, carry):
            source, place, where = peer(i)
            remote(source, place, ts.at[m], tr.at[m], where).start()
            return carry

        source, place, where = peer(0)

        @pl.when(c == core)
        def _():
            pltpu.make_async_copy(source, place, tr.at[m]).start()

        @pl.when(c != core)
        def _():
            remote(source, place, ts.at[m], tr.at[m], where).start()

        lax.fori_loop(1, jump, body, 0, unroll=True)

    def combine(m):
        part = pl.ds(m * slots, slots)
        arrived(ret.at[part], tr.at[m])
        rows = ret[part].astype(F32).reshape(prow, qw).astype(BF16)
        both = dot(gsel[m], rows)
        quarters = both[0 : 4 * tok] + both[4 * tok :]
        return jnp.concatenate([quarters[q * tok : (q + 1) * tok] for q in range(4)], axis=1)

    left, right = pl.ds(0, 2 * qw), pl.ds(2 * qw, 2 * qw)

    def k3_copies():
        return [
            remote(ksend.at[:, left], krecv.at[:, left], k3s.at[0], k3r.at[0], at_z(-jump)),
            remote(ksend.at[:, right], krecv.at[:, right], k3s.at[1], k3r.at[1], at_z(jump)),
        ]

    def kf_copy(i, number, part, where):
        return remote(
            fsend.at[number, :, part], frecv.at[number, :, part], kfs.at[i], kfr.at[i], at_z(where)
        )

    kf_copies = [
        kf_copy(0, 0, right, -jump),
        kf_copy(1, 1, left, jump),
        kf_copy(2, 0, left, -jump),
        kf_copy(3, 1, right, jump),
    ]

    count = pack(0)
    send_local(0)
    for first, second in zip(jumps, onward):
        first.wait_recv()
        second.start()
    pl.when(c == 0)(lambda: gather_1(N0))
    jumps[2].wait_recv()
    count = count + pack(1)
    send_local(1)
    jumps[3].wait_recv()
    count = count + pack(2)
    send_local(2)
    pl.when(c != 0)(lambda: gather_1(N0))
    gather_1(S0)
    gather_1(N12)
    for copy in onward:
        copy.wait_recv()
    count = count + pack(3)
    send_local(3)

    gather_2(N12)
    gather_1(S12)
    gather_1(N3)
    gather_1(S3)
    for copy in weights:
        copy.wait()
    ffn(N0)
    gather_2(S12)
    ffn(N12)
    ffn(N3)
    ffn(S3)
    ffn(S12)
    ffn(S0)

    cnt[...] = count

    def send_count(i, carry):
        s = lax.rem(own + i, slots)
        remote(cnt, crecv.at[lax.rem(s // 2 * 2 + c, slots)], ns, nr, out_peer(s)).start()
        return carry

    pltpu.make_async_copy(cnt, crecv.at[own], nr).start()
    lax.fori_loop(1, slots, send_count, 0)

    reduce_1(N12)
    reduce_2(S3)
    reduce_2(N3)
    reduce_1(S12)
    spread(N0)
    spread(S0)
    reduce_2(N12)
    reduce_2(S12)

    ksend[...] = combine(3).astype(BF16)
    for copy in k3_copies():
        copy.start()
    arrived(crecv, nr)
    csum[...] = jnp.sum(crecv[...], axis=0)
    count_1 = [
        remote(csum, cx.at[0], ncs.at[0], ncr.at[0], at_x(1)),
        remote(csum, cx.at[1], ncs.at[1], ncr.at[1], at_x(-1)),
        remote(csum, cx.at[2], ncs.at[2], ncr.at[2], at_x(2)),
    ]
    for copy in count_1:
        copy.start()
    reduce_2(N0)
    reduce_2(S0)
    near = [combine(1), combine(2)]
    fsend[0, :, 2 * qw :] = near[0][:, 2 * qw :].astype(BF16)
    kf_copies[0].start()
    fsend[1, :, 0 : 2 * qw] = near[1][:, 0 : 2 * qw].astype(BF16)
    kf_copies[1].start()
    k3 = k3_copies()
    k3[0].wait_recv()
    fsend[0, :, 0 : 2 * qw] = (near[0][:, 0 : 2 * qw] + krecv[:, 0 : 2 * qw].astype(F32)).astype(BF16)
    kf_copies[2].start()
    k3[1].wait_recv()
    fsend[1, :, 2 * qw :] = (near[1][:, 2 * qw :] + krecv[:, 2 * qw :].astype(F32)).astype(BF16)
    kf_copies[3].start()
    oparts[...] = combine(0)
    for copy in count_1:
        copy.wait_recv()
    total = csum[...] + cx[0] + cx[1] + cx[2]
    total = total[:, 0:experts] + total[:, experts:]
    loads[...] = total
    for copy in kf_copies:
        copy.wait_recv()
    out[...] = oparts[...] + frecv[0].astype(F32) + frecv[1].astype(F32)

    sends = jumps + onward + k3_copies() + kf_copies + count_1
    for g in range(len(GROUPS)):
        sends += x1_copies(g) + r1_copies(g) + r2_copies(g)
        if g not in DIRECT:
            sends += x2_copies(g)
    for copy in sends:
        copy.wait_send()
    for m in range(4):
        arrived(packed.at[pl.ds(m * slots, slots - 1)], ls.at[m])
        arrived(eo.at[pl.ds(m * slots, slots - 1)], ts.at[m])
    arrived(crecv.at[pl.ds(0, slots - 1)], ns)


def finish(sums, counts, mixed, loads):
    mixed[...] = sums[...].astype(BF16)
    loads[...] = counts[...].astype(jnp.int32)


def per_device(tokens, expert_ids, gate_weights, w_gate, w_up, w_down):
    tok, width = tokens.shape
    hidden = w_gate.shape[2]
    ring = lax.axis_size("ep")
    experts = ring * lax.axis_size("dp")
    slots = 2 * (ring // 4)
    qw = width // 4
    piece = 4 * CAP
    meta = CAP * experts
    prow = slots * piece
    ng = len(GROUPS)
    vmem = pltpu.VMEM
    dma = pltpu.SemaphoreType.DMA
    block = (4 * slots, piece, qw)
    scratch = [
        vmem((tok, width), BF16), vmem(expert_ids.shape[::-1], jnp.int32), vmem(gate_weights.shape[::-1], F32),
        vmem((width, hidden), BF16), vmem((width, hidden), BF16), vmem((width, hidden), BF16),
        vmem((4, tok, width + 2 * meta), BF16),
        vmem(block, BF16),
        vmem((4, *block), BF16),
        vmem((qw // LANES, 4 * prow, LANES), F32),
        vmem((qw // LANES, 4 * 4 * prow, LANES), F32),
        vmem((3, *block), BF16),
        vmem(block, BF16), vmem(block, BF16), vmem(block, BF16), vmem(block, BF16),
        vmem(block, BF16), vmem(block, BF16),
        vmem((4, 8 * tok, prow), BF16),
        vmem((tok, width), F32),
        vmem((tok, width), BF16), vmem((tok, width), BF16),
        vmem((2, tok, width), BF16), vmem((2, tok, width), BF16),
        vmem((1, meta), F32), vmem((slots, 1, meta), F32),
        vmem((1, meta), F32), vmem((3, 1, meta), F32),
        dma((3,)), dma((3,)), dma((6,)), dma((6,)), dma((4,)), dma((8,)),
        dma((ng, 2)), dma((ng, 2)), dma((ng, 2)), dma((ng, 2)),
        dma((ng, 2)), dma((ng, 2)), dma((ng, 2)), dma((ng, 2)),
        dma((4,)), dma((4,)), dma((2,)), dma((2,)), dma((4,)), dma((4,)),
        dma(()), dma(()), dma((3,)), dma((3,)),
    ]
    in_vmem = pl.BlockSpec(memory_space=pltpu.VMEM)
    in_any = pl.BlockSpec(memory_space=pl.ANY)
    sums, counts = pl.pallas_call(
        functools.partial(kernel, ring),
        out_shape=(
            jax.ShapeDtypeStruct((tok, width), F32),
            jax.ShapeDtypeStruct((1, experts), F32),
        ),
        in_specs=[in_any] * 6,
        out_specs=(in_vmem, in_vmem),
        scratch_shapes=scratch,
        compiler_params=pltpu.CompilerParams(
            collective_id=0, has_side_effects=True, vmem_limit_bytes=60 * 1024 * 1024
        ),
        name="routed_ffn",
    )(tokens, expert_ids.T, gate_weights.T, w_gate[0], w_up[0], w_down[0])
    mixed, loads = pl.pallas_call(
        finish,
        out_shape=(
            jax.ShapeDtypeStruct((tok, width), BF16),
            jax.ShapeDtypeStruct((1, experts), jnp.int32),
        ),
        in_specs=[in_vmem, in_vmem],
        out_specs=(in_vmem, in_vmem),
        name="finish",
    )(sums, counts)
    return mixed, loads[0]


def solution(mesh):
    return jax.shard_map(
        per_device,
        mesh=mesh,
        in_specs=(
            P(("groups", "ep", "tp", "dp"), None),
            P(("groups", "ep", "tp", "dp"), None),
            P(("groups", "ep", "tp", "dp"), None),
            P(("ep", "dp"), None, "tp"),
            P(("ep", "dp"), None, "tp"),
            P(("ep", "dp"), None, "tp"),
        ),
        out_specs=(P(("groups", "ep", "tp", "dp"), None), P("groups")),
        check_vma=False,
    )
```

```python
import functools

import jax
import jax.numpy as jnp
from jax import lax
from jax.experimental import pallas as pl
from jax.experimental.pallas import tpu as pltpu
from jax.sharding import PartitionSpec as P

MESH = pl.DeviceIdType.MESH
BF16 = jnp.bfloat16
F32 = jnp.float32
LANES = 128
CAP = 2
N0, S0, N12, N3, S12, S3 = range(6)
GROUPS = ((1, 0, 1), (0, 0, 1), (1, 1, 2), (1, 3, 1), (0, 1, 2), (0, 3, 1))
DIRECT = (N0, S0, N3, S3)


def iota(shape, dim):
    return lax.broadcasted_iota(jnp.int32, shape, dim)


def dot(a, b):
    return jnp.dot(a, b, preferred_element_type=F32)


def dot_nt(a, b):
    return lax.dot_general(a, b, (((1,), (1,)), ((), ())), preferred_element_type=F32)


def kernel(
    ring, tokens_hbm, ids_hbm, gates_hbm, wg_hbm, wu_hbm, wd_hbm, out_hbm, loads_hbm,
    out, loads, tokens, ids, gates, wg, wu, wd, chunk, packed, xrecv, xf, yf, yb, ra, rb, sa, sb, eo, ret,
    gsel, oparts, ksend, krecv, fsend, frecv, cnt, crecv, csum, cx,
    wsem, isem, osem, cs, cr, ls, lr, x1s, x1r, x2s, x2r, r1s, r1r, r2s, r2r,
    ts, tr, k3s, k3r, kfs, kfr, ns, nr, ncs, ncr,
):
    jump = ring // 4
    half = jump // 2
    slots = 2 * jump
    tok, width = tokens.shape
    qw = width // 4
    tiles = qw // LANES
    piece = 4 * CAP
    prow = slots * piece
    lanes = chunk.shape[2] - width
    meta = lanes // 2
    experts = meta // CAP
    top = ids.shape[0]
    cols = (0, qw, 2 * qw + meta, 3 * qw + meta)
    mid = 2 * qw + meta

    z, x, c = lax.axis_index("ep"), lax.axis_index("tp"), lax.axis_index("dp")
    own = (half - c) * 2 + c

    def at_z(d):
        return {"ep": lax.rem(z + d + 2 * ring, ring), "tp": x, "dp": c}

    def at_x(d):
        return {"ep": z, "tp": lax.rem(x + d + 4, 4), "dp": c}

    def out_peer(s):
        return {"ep": lax.rem(z + s // 2 - half + c + ring, ring), "tp": x, "dp": lax.rem(s, 2)}

    def in_peer(s):
        core = lax.rem(s, 2)
        return {"ep": lax.rem(z - s // 2 + half - core + ring, ring), "tp": x, "dp": core}

    def remote(src, dst, send, recv, peer):
        return pltpu.make_async_remote_copy(
            src_ref=src, dst_ref=dst, send_sem=send, recv_sem=recv, device_id=peer, device_id_type=MESH
        )

    def arrived(ref, sem):
        pltpu.make_async_copy(ref, ref, sem).wait()

    weights = [
        pltpu.make_async_copy(src, dst, wsem.at[i])
        for i, (src, dst) in enumerate(((wg_hbm, wg), (wu_hbm, wu), (wd_hbm, wd)))
    ]

    inputs = [
        pltpu.make_async_copy(src, dst, isem.at[i])
        for i, (src, dst) in enumerate(((ids_hbm, ids), (gates_hbm, gates), (tokens_hbm, tokens)))
    ]
    for copy in inputs:
        copy.start()

    barrier = pltpu.get_barrier_semaphore()

    def greet(peer):
        pl.semaphore_signal(barrier, inc=1, device_id=peer, device_id_type=MESH)

    greet(at_z(jump))
    greet(at_z(-jump))
    for d in (1, -1, 2):
        greet(at_x(d))
    greet({"ep": z, "tp": x, "dp": 1 - c})
    for d in range(1, half):
        for step in (d, -d):
            for core in range(2):
                greet({"ep": lax.rem(z + step + ring, ring), "tp": x, "dp": core})
    greet({"ep": lax.rem(z + half, ring), "tp": x, "dp": 0})
    greet({"ep": lax.rem(z - half + ring, ring), "tp": x, "dp": 1})
    greet({"ep": lax.rem(z + (2 * c - 1) * half + ring, ring), "tp": x, "dp": c})
    for copy in weights:
        copy.start()

    for copy in inputs:
        copy.wait()

    line = iota((meta, tok), 0)
    line_expert = jnp.where(line >= experts, line - experts, line)
    line_rank = jnp.where(line >= experts, 1.0, 0.0)
    hit = jnp.zeros((meta, tok), F32)
    gate = jnp.zeros((meta, tok), F32)
    for k in range(top):
        same = ids[k : k + 1, :] == line_expert
        hit = hit + jnp.where(same, 1.0, 0.0)
        gate = gate + jnp.where(same, gates[k : k + 1, :], 0.0)
    row, column = iota((tok, tok), 0), iota((tok, tok), 1)
    rank = dot(hit.astype(BF16), jnp.where(row < column, 1.0, 0.0).astype(BF16))
    gate = jnp.where(rank == line_rank, gate, 0.0)
    gate_hi = gate.astype(BF16)
    gate_lo = (gate - gate_hi.astype(F32)).astype(BF16)
    unit = jnp.where(row == column, 1.0, 0.0).astype(BF16)
    gate_hi = dot_nt(unit, gate_hi).astype(BF16)
    gate_lo = dot_nt(unit, gate_lo).astype(BF16)
    chunk[0, :, 0 : 2 * qw] = tokens[:, 0 : 2 * qw]
    chunk[0, :, 2 * qw : mid] = gate_hi
    chunk[0, :, mid : mid + 2 * qw] = tokens[:, 2 * qw :]
    chunk[0, :, mid + 2 * qw :] = gate_lo

    pl.semaphore_wait(barrier, 4 * half + 5)

    low, high = pl.ds(0, mid), pl.ds(mid, mid)

    def jump_copy(i, part, source, target, where):
        return remote(
            chunk.at[source, :, part], chunk.at[target, :, part], cs.at[i], cr.at[i], at_z(where)
        )

    jumps = [
        jump_copy(0, low, 0, 1, jump),
        jump_copy(1, high, 0, 2, -jump),
        jump_copy(2, high, 0, 1, jump),
        jump_copy(3, low, 0, 2, -jump),
    ]
    onward = [jump_copy(4, low, 1, 3, jump), jump_copy(5, high, 2, 3, -jump)]
    for copy in jumps:
        copy.start()

    row = iota((prow, meta), 0)
    lane = iota((prow, meta), 1)
    row_slot = row // piece
    row_z = lax.rem(z + row_slot // 2 - half + c + ring, ring)
    row_expert = row_z * 2 + lax.rem(row_slot, 2)
    row_rank = lax.rem(row // 4, CAP)
    pick = jnp.where(row_rank * experts + row_expert == lane, 1.0, 0.0).astype(BF16)
    quarter_r = lax.rem(iota((prow, 4 * tok), 0), 4) == iota((prow, 4 * tok), 1) // tok
    quarter_c = lax.rem(iota((4 * tok, prow), 1), 4) == iota((4 * tok, prow), 0) // tok

    def pack(m):
        hi = chunk[m, :, 2 * qw : mid]
        lo = chunk[m, :, mid + 2 * qw :]
        used = jnp.where(hi.astype(F32) > 0.0, 1.0, 0.0)
        count = jnp.sum(used, axis=0, keepdims=True)
        used = used.astype(BF16)
        select = dot_nt(pick, jnp.concatenate([used] * 4, axis=0))
        select = jnp.where(quarter_r, select, 0.0).astype(BF16)
        quarters = jnp.concatenate([chunk[m, :, o : o + qw] for o in cols], axis=0)
        rows = dot(select, quarters).astype(BF16)
        packed[pl.ds(m * slots, slots)] = rows.reshape(slots, piece, qw)
        for h, part in enumerate((hi, lo)):
            mix = dot_nt(jnp.concatenate([part] * 4, axis=0), pick)
            gsel[m, pl.ds(h * 4 * tok, 4 * tok), :] = jnp.where(quarter_c, mix, 0.0).astype(BF16)
        return count

    def send_local(m):
        def body(i, carry):
            s = lax.rem(own + i, slots)
            remote(
                packed.at[m * slots + s],
                xrecv.at[0, (c * 4 + m) * jump + s // 2],
                ls.at[m], lr.at[c * 4 + m], out_peer(s),
            ).start()
            return carry

        here = xrecv.at[0, (c * 4 + m) * jump + own // 2]
        pltpu.make_async_copy(packed.at[m * slots + own], here, lr.at[c * 4 + m]).start()
        lax.fori_loop(1, slots, body, 0, unroll=True)

    def span(g):
        core, m0, nm = GROUPS[g]
        return (core * 4 + m0) * jump, nm * jump

    def halves(g):
        s0, n = span(g)
        return pl.ds(s0, n // 2), pl.ds(s0 + n // 2, n // 2)

    def x1_copies(g):
        s0, n = span(g)
        part = xrecv.at[0, pl.ds(s0, n)]
        return [
            remote(part, xrecv.at[2, pl.ds(s0, n)], x2s.at[g, 0], x2r.at[g, 0], at_x(2)),
            remote(part, xrecv.at[1, pl.ds(s0, n)], x1s.at[g, 0], x1r.at[g, 0], at_x(1)),
            remote(part, xrecv.at[3, pl.ds(s0, n)], x1s.at[g, 1], x1r.at[g, 1], at_x(-1)),
        ]

    def gather_1(g):
        core, m0, nm = GROUPS[g]
        for n in range(core * 4 + m0, core * 4 + m0 + nm):
            arrived(xrecv.at[0, pl.ds(n * jump, jump)], lr.at[n])
        for copy in x1_copies(g):
            copy.start()

    def ffn(g):
        s0, n = span(g)
        count = 4 * n * piece
        rows = count // 4
        for copy in x1_copies(g):
            copy.wait_recv()
        for j in range(tiles):
            arrivals = xrecv[:, pl.ds(s0, n), :, j * LANES : (j + 1) * LANES]
            xf[j, pl.ds(0, count)] = arrivals.astype(F32).reshape(count, LANES)
        full = jnp.concatenate(
            [
                xf[j, pl.ds(q, rows, stride=4), :].astype(BF16)
                for q in range(4)
                for j in range(tiles)
            ],
            axis=1,
        )
        gate_value = dot(full, wg[...])
        up_value = dot(full, wu[...])
        hidden = (gate_value / (1.0 + jnp.exp(-gate_value)) * up_value).astype(BF16)
        for q in range(4):
            terms = dot_nt(hidden, wd[pl.ds(q * qw, qw), :])
            for j in range(tiles):
                place = pl.ds(4 * s0 * piece + q, rows, stride=4)
                yf[j, place, :] = terms[:, j * LANES : (j + 1) * LANES]
        if g not in (N0, S0):
            spread(g)

    def spread(g):
        s0, n = span(g)
        part = pl.ds(s0, n)
        yb[1, part] = partial(g, 2, 0, n).astype(BF16)
        for copy in r1_copies(g):
            copy.start()
        if g in DIRECT:
            yb[2, part] = partial(g, 3, 0, n).astype(BF16)
            yb[0, part] = partial(g, 1, 0, n).astype(BF16)
            for copy in r2_copies(g):
                copy.start()

    def partial(g, column, first, number):
        s0, n = span(g)
        start = (4 * s0 + column * n + first) * piece
        parts = [yf[j, pl.ds(start, number * piece), :] for j in range(tiles)]
        return jnp.concatenate(parts, axis=1).reshape(number, piece, qw)

    def r1_copies(g):
        a, b = halves(g)
        if g in DIRECT:
            s0, n = span(g)
            part = pl.ds(s0, n)
            return [remote(yb.at[1, part], ra.at[part], r1s.at[g, 0], r1r.at[g, 0], at_x(2))]
        return [
            remote(yb.at[1, a], ra.at[a], r1s.at[g, 0], r1r.at[g, 0], at_x(1)),
            remote(yb.at[1, b], rb.at[b], r1s.at[g, 1], r1r.at[g, 1], at_x(-1)),
        ]

    def r2_copies(g):
        s0, n = span(g)
        part = pl.ds(s0, n)
        return [
            remote(yb.at[2, part], sa.at[part], r2s.at[g, 0], r2r.at[g, 0], at_x(1)),
            remote(yb.at[0, part], sb.at[part], r2s.at[g, 1], r2r.at[g, 1], at_x(-1)),
        ]

    def reduce_1(g):
        s0, n = span(g)
        a, b = halves(g)
        one, two = r1_copies(g), r2_copies(g)
        yb[2, b] = partial(g, 3, n // 2, n // 2).astype(BF16)
        yb[0, a] = partial(g, 1, 0, n // 2).astype(BF16)
        one[0].wait_recv()
        yb[2, a] = (partial(g, 3, 0, n // 2) + ra[a].astype(F32)).astype(BF16)
        two[0].start()
        one[1].wait_recv()
        yb[0, b] = (partial(g, 1, n // 2, n // 2) + rb[b].astype(F32)).astype(BF16)
        two[1].start()

    def reduce_2(g):
        core, m0, nm = GROUPS[g]
        s0, n = span(g)
        part = pl.ds(s0, n)
        for copy in r2_copies(g):
            copy.wait_recv()
        total = partial(g, 0, 0, n) + sa[part].astype(F32) + sb[part].astype(F32)
        if g in DIRECT:
            for copy in r1_copies(g):
                copy.wait_recv()
            total = total + ra[part].astype(F32)
        eo[part] = total.astype(BF16)
        for m in range(m0, m0 + nm):
            send_back(core, m)

    def send_back(core, m):
        def peer(i):
            n = lax.rem(half - core + i, jump)
            source = eo.at[(core * 4 + m) * jump + n]
            place = ret.at[m * slots + n * 2 + c]
            where = {"ep": lax.rem(z - n + half - core + ring, ring), "tp": x, "dp": core}
            return source, place, where

        def body(i, carry):
            source, place, where = peer(i)
            remote(source, place, ts.at[m], tr.at[m], where).start()
            return carry

        source, place, where = peer(0)

        @pl.when(c == core)
        def _():
            pltpu.make_async_copy(source, place, tr.at[m]).start()

        @pl.when(c != core)
        def _():
            remote(source, place, ts.at[m], tr.at[m], where).start()

        lax.fori_loop(1, jump, body, 0, unroll=True)

    def combine(m):
        part = pl.ds(m * slots, slots)
        arrived(ret.at[part], tr.at[m])
        rows = ret[part].astype(F32).reshape(prow, qw).astype(BF16)
        both = dot(gsel[m], rows)
        quarters = both[0 : 4 * tok] + both[4 * tok :]
        return jnp.concatenate([quarters[q * tok : (q + 1) * tok] for q in range(4)], axis=1)

    left, right = pl.ds(0, 2 * qw), pl.ds(2 * qw, 2 * qw)

    def k3_copies():
        return [
            remote(ksend.at[:, left], krecv.at[:, left], k3s.at[0], k3r.at[0], at_z(-jump)),
            remote(ksend.at[:, right], krecv.at[:, right], k3s.at[1], k3r.at[1], at_z(jump)),
        ]

    def kf_copy(i, number, part, where):
        return remote(
            fsend.at[number, :, part], frecv.at[number, :, part], kfs.at[i], kfr.at[i], at_z(where)
        )

    kf_copies = [
        kf_copy(0, 0, right, -jump),
        kf_copy(1, 1, left, jump),
        kf_copy(2, 0, left, -jump),
        kf_copy(3, 1, right, jump),
    ]

    count = pack(0)
    send_local(0)
    for first, second in zip(jumps, onward):
        first.wait_recv()
        second.start()
    pl.when(c == 0)(lambda: gather_1(N0))
    jumps[2].wait_recv()
    count = count + pack(1)
    send_local(1)
    jumps[3].wait_recv()
    count = count + pack(2)
    send_local(2)
    pl.when(c != 0)(lambda: gather_1(N0))
    gather_1(S0)
    gather_1(N12)
    for copy in onward:
        copy.wait_recv()
    count = count + pack(3)
    send_local(3)

    for copy in weights:
        copy.wait()
    ffn(N0)
    gather_1(S12)
    gather_1(N3)
    gather_1(S3)
    ffn(N12)
    ffn(S12)
    ffn(N3)
    ffn(S3)
    reduce_1(N12)
    reduce_1(S12)
    ffn(S0)

    cnt[...] = count

    def send_count(i, carry):
        s = lax.rem(own + i, slots)
        remote(cnt, crecv.at[lax.rem(s // 2 * 2 + c, slots)], ns, nr, out_peer(s)).start()
        return carry

    pltpu.make_async_copy(cnt, crecv.at[own], nr).start()
    lax.fori_loop(1, slots, send_count, 0)

    reduce_2(S3)
    reduce_2(N3)
    spread(N0)
    spread(S0)
    reduce_2(N12)
    reduce_2(S12)

    ksend[...] = combine(3).astype(BF16)
    for copy in k3_copies():
        copy.start()
    arrived(crecv, nr)
    csum[...] = jnp.sum(crecv[...], axis=0)
    count_1 = [
        remote(csum, cx.at[0], ncs.at[0], ncr.at[0], at_x(1)),
        remote(csum, cx.at[1], ncs.at[1], ncr.at[1], at_x(-1)),
        remote(csum, cx.at[2], ncs.at[2], ncr.at[2], at_x(2)),
    ]
    for copy in count_1:
        copy.start()
    reduce_2(N0)
    reduce_2(S0)
    near = [combine(1), combine(2)]
    fsend[0, :, 2 * qw :] = near[0][:, 2 * qw :].astype(BF16)
    kf_copies[0].start()
    fsend[1, :, 0 : 2 * qw] = near[1][:, 0 : 2 * qw].astype(BF16)
    kf_copies[1].start()
    k3 = k3_copies()
    k3[0].wait_recv()
    fsend[0, :, 0 : 2 * qw] = (near[0][:, 0 : 2 * qw] + krecv[:, 0 : 2 * qw].astype(F32)).astype(BF16)
    kf_copies[2].start()
    k3[1].wait_recv()
    fsend[1, :, 2 * qw :] = (near[1][:, 2 * qw :] + krecv[:, 2 * qw :].astype(F32)).astype(BF16)
    kf_copies[3].start()
    oparts[...] = combine(0)
    for copy in count_1:
        copy.wait_recv()
    total = csum[...] + cx[0] + cx[1] + cx[2]
    total = total[:, 0:experts] + total[:, experts:]
    loads[...] = total.astype(jnp.int32)
    loads_out = pltpu.make_async_copy(loads, loads_hbm, osem.at[0])
    loads_out.start()
    for copy in kf_copies:
        copy.wait_recv()
    out[...] = (oparts[...] + frecv[0].astype(F32) + frecv[1].astype(F32)).astype(BF16)
    mixed_out = pltpu.make_async_copy(out, out_hbm, osem.at[1])
    mixed_out.start()

    sends = jumps + onward + k3_copies() + kf_copies + count_1
    for g in range(len(GROUPS)):
        sends += x1_copies(g) + r1_copies(g) + r2_copies(g)
    for copy in sends:
        copy.wait_send()
    for m in range(4):
        arrived(packed.at[pl.ds(m * slots, slots - 1)], ls.at[m])
        arrived(eo.at[pl.ds(m * slots, slots - 1)], ts.at[m])
    arrived(crecv.at[pl.ds(0, slots - 1)], ns)
    loads_out.wait()
    mixed_out.wait()


def finish(sums, counts, mixed, loads):
    mixed[...] = sums[...]
    loads[...] = counts[...]


def per_device(tokens, expert_ids, gate_weights, w_gate, w_up, w_down):
    tok, width = tokens.shape
    hidden = w_gate.shape[2]
    ring = lax.axis_size("ep")
    experts = ring * lax.axis_size("dp")
    slots = 2 * (ring // 4)
    qw = width // 4
    piece = 4 * CAP
    meta = CAP * experts
    prow = slots * piece
    ng = len(GROUPS)
    vmem = pltpu.VMEM
    dma = pltpu.SemaphoreType.DMA
    block = (4 * slots, piece, qw)
    scratch = [
        vmem((tok, width), BF16), vmem((1, experts), jnp.int32),
        vmem((tok, width), BF16), vmem(expert_ids.shape[::-1], jnp.int32), vmem(gate_weights.shape[::-1], F32),
        vmem((width, hidden), BF16), vmem((width, hidden), BF16), vmem((width, hidden), BF16),
        vmem((4, tok, width + 2 * meta), BF16),
        vmem(block, BF16),
        vmem((4, *block), BF16),
        vmem((qw // LANES, 4 * prow, LANES), F32),
        vmem((qw // LANES, 4 * 4 * prow, LANES), F32),
        vmem((3, *block), BF16),
        vmem(block, BF16), vmem(block, BF16), vmem(block, BF16), vmem(block, BF16),
        vmem(block, BF16), vmem(block, BF16),
        vmem((4, 8 * tok, prow), BF16),
        vmem((tok, width), F32),
        vmem((tok, width), BF16), vmem((tok, width), BF16),
        vmem((2, tok, width), BF16), vmem((2, tok, width), BF16),
        vmem((1, meta), F32), vmem((slots, 1, meta), F32),
        vmem((1, meta), F32), vmem((3, 1, meta), F32),
        dma((3,)), dma((3,)), dma((2,)), dma((6,)), dma((6,)), dma((4,)), dma((8,)),
        dma((ng, 2)), dma((ng, 2)), dma((ng, 2)), dma((ng, 2)),
        dma((ng, 2)), dma((ng, 2)), dma((ng, 2)), dma((ng, 2)),
        dma((4,)), dma((4,)), dma((2,)), dma((2,)), dma((4,)), dma((4,)),
        dma(()), dma(()), dma((3,)), dma((3,)),
    ]
    in_vmem = pl.BlockSpec(memory_space=pltpu.VMEM)
    in_any = pl.BlockSpec(memory_space=pl.ANY)
    sums, counts = pl.pallas_call(
        functools.partial(kernel, ring),
        out_shape=(
            jax.ShapeDtypeStruct((tok, width), BF16),
            jax.ShapeDtypeStruct((1, experts), jnp.int32),
        ),
        in_specs=[in_any] * 6,
        out_specs=(in_any, in_any),
        scratch_shapes=scratch,
        compiler_params=pltpu.CompilerParams(
            collective_id=0, has_side_effects=True, vmem_limit_bytes=60 * 1024 * 1024
        ),
        name="routed_ffn",
    )(tokens, expert_ids.T, gate_weights.T, w_gate[0], w_up[0], w_down[0])
    mixed, loads = pl.pallas_call(
        finish,
        out_shape=(
            jax.ShapeDtypeStruct((tok, width), BF16),
            jax.ShapeDtypeStruct((1, experts), jnp.int32),
        ),
        in_specs=[in_vmem, in_vmem],
        out_specs=(in_vmem, in_vmem),
        name="finish",
    )(sums, counts)
    return mixed, loads[0]


def solution(mesh):
    return jax.shard_map(
        per_device,
        mesh=mesh,
        in_specs=(
            P(("groups", "ep", "tp", "dp"), None),
            P(("groups", "ep", "tp", "dp"), None),
            P(("groups", "ep", "tp", "dp"), None),
            P(("ep", "dp"), None, "tp"),
            P(("ep", "dp"), None, "tp"),
            P(("ep", "dp"), None, "tp"),
        ),
        out_specs=(P(("groups", "ep", "tp", "dp"), None), P("groups")),
        check_vma=False,
    )
```
